256 devices in a mesh: groups: 4 (over y, x), ctx: 32 (over z), tp: 2 (over core).
Axes of the slice: x: 2, y: 2, z: 32, core: 2. Of those that a mesh axis runs over, the one named last changes fastest.
The devices are a block of a 4x8x32 slice.
Arguments:
- query_states: bfloat16 [32768, 32, 128], P(('groups', 'ctx'), 'tp'), parts along dimension 0, may hold values from -8 to 8
- key_states: bfloat16 [32768, 4, 128], P(('groups', 'ctx'), 'tp'), parts along dimension 0, may hold values from -8 to 8
- value_rows: bfloat16 [32768, 4, 128], P(('groups', 'ctx'), 'tp'), parts along dimension 0, may hold values from -12 to 12
- positions: int32 [32768], P(('groups', 'ctx')), parts along dimension 0, may hold values from 0 to 8191, as said below
- out_weight: bfloat16 [4096, 4096], P('tp', 'ctx'), may hold values from -0.375 to 0.375
Outputs:
- projected: bfloat16 [32768, 4096], P(('groups', 'ctx'), 'tp'), parts along dimension 0
The draws below stay inside these ranges and needn't reach their ends.
There are 4 independent parts, one for each index of `groups`. The reference program is written for one: setup_inputs(seed, part) draws one part's arguments, and reference() takes and returns one part's arrays. A program takes and returns all parts, laid end to end along the dimension named above; an argument that names none is the same for every part. Nothing has to cross between parts.
Inputs may be any that keep to these rules, and one draw needn't show every extreme that they name: Each of 0 to 8191 appears once. Half-block b holds positions b * 128 to (b + 1) * 128 - 1. The 256 rows of one device along ctx hold half-block j and then half-block 64 - 1 - j, each in rising order, for a j below 32 that differs from device to device.
All inputs are finite; a program needn't handle non-finite values.
Results may differ from the reference program's by a relative error of at most 0.01.
Values may be sent and summed in bfloat16 or wider, within the bound.
No kernel may reach another device: no remote copies, remote signals or barrier semaphores. Data moves between devices by JAX's collectives and lax.ppermute only.
A program may use at most 64 MiB of HBM per device.

```python
from functools import partial
import jax
import jax.numpy as jnp
from jax import lax

QUERY_HEAD_COUNT = 32
KEY_VALUE_HEADS = 4
HEAD_WIDTH = 128
DOUT = 4096
HALF = 128
SEQUENCE_LENGTH = 8192
HALF_BLOCK_COUNT = 64


def draw_query_states(key, part):
    base_point = jax.random.fold_in(key, 21)
    value_entries = jnp.clip(jax.random.normal(jax.random.fold_in(base_point, 1), (SEQUENCE_LENGTH, QUERY_HEAD_COUNT, HEAD_WIDTH)), -8.0, 8.0)
    return value_entries.astype(jnp.bfloat16)


def draw_key_states(key, part):
    base_point = jax.random.fold_in(key, 41)
    value_entries = jnp.clip(jax.random.normal(jax.random.fold_in(base_point, 1), (SEQUENCE_LENGTH, KEY_VALUE_HEADS, HEAD_WIDTH)), -8.0, 8.0)
    return value_entries.astype(jnp.bfloat16)


def draw_positions(key, part):
    order = jax.random.permutation(jax.random.fold_in(key, 31), HALF_BLOCK_COUNT // 2)
    within = jnp.arange(HALF)
    lower = order[:, None] * HALF + within[None, :]
    upper = (HALF_BLOCK_COUNT - 1 - order)[:, None] * HALF + within[None, :]
    return jnp.concatenate([lower, upper], axis=1).reshape(SEQUENCE_LENGTH).astype(jnp.int32)


def steps_of(stream_key, dims, cuts, low, top_value):
    loudness = 1.0
    for dim, parts in cuts:
        steps = jax.random.uniform(jax.random.fold_in(jax.random.fold_in(stream_key, 6), dim), (parts,), jnp.float32, low / len(cuts), top_value / len(cuts))
        loudness = loudness * jnp.repeat(jnp.exp(steps), dims[dim] // parts).reshape((-1,) + (1,) * (len(dims) - 1 - dim))
    return loudness


def gaussian(key, shape, scale, limit, shards=(), dtype=jnp.bfloat16):
    loudness = steps_of(key, shape, shards, -0.22, 0.18) if shards else 1.0
    values = jax.random.normal(key, shape, jnp.float32) * scale * loudness
    return jnp.minimum(jnp.maximum(values, -limit), limit).astype(dtype)


def setup_inputs(seed: int = 0, part: int = 0) -> dict:
    streams_of = jax.random.split(jax.random.key(seed), 6)
    part_splits = jax.random.split(jax.random.fold_in(streams_of[5], part), 6)
    query_states = draw_query_states(jax.random.fold_in(jax.random.fold_in(streams_of[5], part), 71), part)
    key_states = draw_key_states(jax.random.fold_in(jax.random.fold_in(streams_of[5], part), 71), part)
    value_rows = gaussian(part_splits[2], (SEQUENCE_LENGTH, KEY_VALUE_HEADS, HEAD_WIDTH), 2.0, 12.0, ((0, 32), (1, 2)))
    positions = draw_positions(jax.random.fold_in(jax.random.fold_in(streams_of[5], part), 71), part)
    out_weight = gaussian(streams_of[4], (QUERY_HEAD_COUNT * HEAD_WIDTH, DOUT), (QUERY_HEAD_COUNT * HEAD_WIDTH // 16) ** -0.5, 0.375, ((0, 2), (1, 32)))
    return {"query_states": query_states, "key_states": key_states, "value_rows": value_rows, "positions": positions, "out_weight": out_weight}


def one_head(operands, visible):
    query_head, key_head, value_head = operands
    scores = jnp.dot(query_head, key_head.T, preferred_element_type=jnp.float32) * (HEAD_WIDTH ** -0.5)
    scores = jnp.where(visible, scores, -jnp.inf)
    largest = jnp.max(scores, axis=1)
    exp_scores = jnp.exp(scores - largest[:, None])
    denominator = jnp.sum(exp_scores, axis=1)
    weighted = jnp.dot(exp_scores.astype(jnp.bfloat16), value_head, preferred_element_type=jnp.float32)
    return (weighted / denominator[:, None]).astype(jnp.bfloat16)


def reference(query_states, key_states, value_rows, positions, out_weight):
    visible = positions[None, :] <= positions[:, None]
    group_width = QUERY_HEAD_COUNT // KEY_VALUE_HEADS
    query_major = jnp.moveaxis(query_states, 1, 0)
    key_major = jnp.repeat(jnp.moveaxis(key_states, 1, 0), group_width, axis=0)
    value_major = jnp.repeat(jnp.moveaxis(value_rows, 1, 0), group_width, axis=0)
    attended = lax.map(partial(one_head, visible=visible), (query_major, key_major, value_major))
    attended = jnp.moveaxis(attended, 0, 1).reshape(SEQUENCE_LENGTH, QUERY_HEAD_COUNT * HEAD_WIDTH)
    return jnp.dot(attended, out_weight, preferred_element_type=jnp.float32).astype(jnp.bfloat16)
```

```python
import functools
import math

import jax
import jax.numpy as jnp
from jax import lax
from jax.experimental import pallas as pl
from jax.experimental.pallas import tpu as pltpu
from jax.sharding import PartitionSpec as P


LOW_START = -1e30
TAG_ROWS = 16
LANES = 256
BF16 = jnp.bfloat16
F32 = jnp.float32


def chunk_ends(steps):
    return [*range(1, steps - 2, 3), steps - 1, steps]


def batch_ends(steps):
    return [*range(2, steps - 1, 2), steps - 1, steps]


def attend_kernel(first, blocks, half, scale, *refs):
    own_ref, q_ref = refs[:2]
    at = 2
    if not first:
        acc_in, max_in, sum_in = refs[at : at + 3]
        at += 3
    packs = refs[at : at + blocks]
    at += blocks
    acc, largest, total, held, sem = refs[at:]
    head = pl.program_id(0)
    rows = held.shape[2]
    span = q_ref.shape[1] // 2

    def copy(h, b):
        return pltpu.make_async_copy(
            packs[b].at[pl.ds(h * rows, rows)], held.at[h, b], sem.at[h, b]
        )

    @pl.when(head == 0)
    def _():
        for h in range(2):
            for b in range(blocks):
                copy(h, b).start()

    if first:
        acc[...] = jnp.zeros_like(acc)
        largest[...] = jnp.full_like(largest, LOW_START)
        total[...] = jnp.zeros_like(total)
    else:
        acc[...] = acc_in[...]
        largest[...] = max_in[...]
        total[...] = sum_in[...]

    for h in range(2):

        @pl.when(head == h)
        def _():
            for b in range(blocks):
                copy(h, b).wait()

    def update(tiles, mask=None):
        found = []
        for start, keys, values in tiles:
            lanes = pl.ds(pl.multiple_of(start, LANES), LANES)
            scores = lax.dot_general(
                keys, q_ref[0, lanes, :], (((1,), (1,)), ((), ())), preferred_element_type=F32
            )
            if mask is not None:
                scores = jnp.where(mask, scores, LOW_START)
            old = largest[0, 0:1, lanes]
            new = jnp.maximum(old, jnp.max(scores, axis=0, keepdims=True))
            factor = jnp.exp2((old - new) * scale)
            weights = jnp.exp2((scores - new) * scale)
            summed = total[0, :, lanes] * factor + jnp.sum(
                weights.reshape(weights.shape[0] // 8, 8, LANES), axis=0
            )
            weighted = acc[0, :, lanes] * factor + lax.dot_general(
                values,
                weights.astype(BF16),
                (((0,), (0,)), ((), ())),
                preferred_element_type=F32,
            )
            found.append((lanes, summed, weighted, jnp.broadcast_to(new, (8, LANES))))
        for lanes, summed, weighted, new in found:
            total[0, :, lanes] = summed
            acc[0, :, lanes] = weighted
            largest[0, :, lanes] = new

    low, high = pl.ds(0, half), pl.ds(half, half)
    vlow, vhigh = pl.ds(2 * half, half), pl.ds(3 * half, half)
    tiles = span // LANES
    if first:
        mine = held.at[head, 0]
        place_k = lax.broadcasted_iota(jnp.int32, (half, LANES), 0)
        place_q = lax.broadcasted_iota(jnp.int32, (half, LANES), 1) % half
        mask = place_k <= place_q

        def visit_own(j, carry):
            at = j * LANES
            update([(at, mine[low], mine[vlow]), (span + at, mine[high], mine[vhigh])], mask)
            update([(span + at, mine[low], mine[vlow])])
            return carry

        lax.fori_loop(0, tiles, visit_own, 0)
        return

    def visit(b, carry):
        block = held.at[head, b]
        tag = jnp.max(block[pl.ds(4 * half, TAG_ROWS)].astype(F32))
        ahead = tag < own_ref[0].astype(F32)
        key_at = pl.multiple_of(jnp.where(ahead, 0, half), half)
        lane_at = jnp.where(ahead, 0, span)

        def some(i, carry):
            work = []
            for j in range(tiles // 2):
                near = (i * (tiles // 2) + j) * LANES
                far = ((1 - i) * (tiles // 2) + j) * LANES
                work.append((span + near, block[low], block[vlow]))
                work.append(
                    (
                        lane_at + far,
                        block[pl.ds(key_at, half)],
                        block[pl.ds(2 * half + key_at, half)],
                    )
                )
            update(work)
            return carry

        return lax.fori_loop(0, 2, some, carry)

    lax.fori_loop(0, blocks, visit, 0)


def attend(own, grouped, state, packs, half):
    first = state is None
    heads, lanes, width = grouped.shape
    blocks = len(packs)
    per_head = lambda *dims: pl.BlockSpec((1, *dims), lambda h: (h, 0, 0))
    anywhere = pl.BlockSpec(memory_space=pl.ANY)
    state_specs = [per_head(width, lanes), per_head(8, lanes), per_head(8, lanes)]
    state_shapes = [
        jax.ShapeDtypeStruct((heads, width, lanes), F32),
        jax.ShapeDtypeStruct((heads, 8, lanes), F32),
        jax.ShapeDtypeStruct((heads, 8, lanes), F32),
    ]
    rows = 4 * half + TAG_ROWS
    flops = heads * blocks * 2 * half * (lanes // 2) * width * 4
    return pl.pallas_call(
        functools.partial(attend_kernel, first, blocks, half, width**-0.5 * math.log2(math.e)),
        grid=(heads,),
        in_specs=[pl.BlockSpec(memory_space=pltpu.SMEM), per_head(lanes, width)]
        + ([] if first else state_specs)
        + [anywhere] * blocks,
        out_specs=state_specs,
        out_shape=state_shapes,
        scratch_shapes=[
            pltpu.VMEM((heads, blocks, rows, width), BF16),
            pltpu.SemaphoreType.DMA((heads, blocks)),
        ],
        input_output_aliases={} if first else {2: 0, 3: 1, 4: 2},
        cost_estimate=pl.CostEstimate(
            flops=flops, transcendentals=flops // (4 * width), bytes_accessed=6 << 20
        ),
        compiler_params=pltpu.CompilerParams(
            vmem_limit_bytes=24 << 20, dimension_semantics=("arbitrary",)
        ),
    )(own, grouped, *(() if first else state), *packs)


def project_kernel(chunks, steps, ring, *refs):
    info, acc, total, own_weight = refs[:4]
    pieces = refs[4 : 4 + 5 * len(chunks)]
    mine, theirs, attended, weights, out, sem, out_sem = refs[4 + 5 * len(chunks) :]
    me, core, spot = info[0], info[1], info[2]
    eighths, rows, depth = attended.shape
    width = weights.shape[-1]
    half = rows // 2
    quarter = [spot, spot ^ 1, spot ^ 2, spot ^ 3]

    def copies(k):
        first_step, last_step = chunks[k]
        forward = last_step - first_step + 1
        backward = min(last_step, steps - 1) - first_step + 1
        own_part, x_part, y_part, x_relay, y_relay = pieces[5 * k : 5 * k + 5]
        found = []
        for source, q, parts in [
            (own_part, 0, (0, 1)),
            (x_part, 1, (0, 1)),
            (y_part, 2, (0, 1)),
            (x_relay, 3, (0,)),
            (y_relay, 3, (1,)),
        ]:
            for part in parts:
                for n, at, to in (
                    (forward, 0, first_step - 1),
                    (backward, forward, steps + first_step - 1),
                ):
                    if n:
                        held = source.at[part] if len(parts) == 2 else source
                        found.append(
                            pltpu.make_async_copy(
                                held.at[pl.ds(at, n)],
                                weights.at[pl.ds(to, n), quarter[q] * 2 + part],
                                sem.at[k],
                            )
                        )
        return found

    own_copy = pltpu.make_async_copy(own_weight, weights.at[2 * steps - 1], sem.at[len(chunks)])
    own_copy.start()
    for k in range(len(chunks)):
        for copy in copies(k):
            copy.start()

    heads, _, lanes = acc.shape
    span = lanes // 2
    for h in range(heads):
        for s in range(2):
            for g in range(span // half):
                at = pl.ds(s * span + g * half, half)
                whole = jnp.sum(total[h, :, at], axis=0, keepdims=True)
                value = (acc[h, :, at] / whole).T.astype(BF16)
                head = h * (span // half) + g
                per = depth // value.shape[1]
                attended[
                    head // per,
                    pl.ds(s * half, half),
                    pl.ds((head % per) * value.shape[1], value.shape[1]),
                ] = value
    own_copy.wait()

    def step(i, carry):
        for k, (first_step, _) in enumerate(chunks):

            @pl.when(i == first_step - 1)
            def _():
                for copy in copies(k):
                    copy.wait()

        summed = jnp.zeros((rows, 2 * width), F32)
        for e in range(eighths):
            both = jnp.concatenate([weights[i, e], weights[steps + i, e]], axis=1)
            summed += jnp.dot(attended[e], both, preferred_element_type=F32)
        rounded = summed.astype(BF16)
        ahead = lax.rem(me - (i + 1) + ring, ring)
        behind = jnp.where(i == steps - 1, me, lax.rem(me + i + 1, ring))
        for value, block in ((rounded[:, :width], ahead), (rounded[:, width:], behind)):
            side = block // (ring // 2)
            at = pl.multiple_of((block - side * (ring // 2)) * width, width)
            out[side ^ core, :, pl.ds(at, width)] = value
        return carry

    lax.fori_loop(0, steps, step, 0)
    done = [
        pltpu.make_async_copy(out.at[0], mine, out_sem.at[0]),
        pltpu.make_async_copy(out.at[1], theirs, out_sem.at[1]),
    ]
    for copy in done:
        copy.start()
    for copy in done:
        copy.wait()


def project(info, state, own_weight, pieces, chunks, steps, ring):
    acc, _, total = state
    heads, width, lanes = acc.shape
    eighths, depth, columns = own_weight.shape
    rows = heads * lanes * width // (eighths * depth)
    out_columns = columns * ring // 2
    anywhere = pl.BlockSpec(memory_space=pl.ANY)
    vmem = pl.BlockSpec(memory_space=pltpu.VMEM)
    flat = [array for chunk in pieces for array in chunk]
    return pl.pallas_call(
        functools.partial(project_kernel, chunks, steps, ring),
        in_specs=[pl.BlockSpec(memory_space=pltpu.SMEM), vmem, vmem]
        + [anywhere] * (1 + len(flat)),
        out_specs=[anywhere, anywhere],
        out_shape=[jax.ShapeDtypeStruct((rows, out_columns), BF16)] * 2,
        scratch_shapes=[
            pltpu.VMEM((eighths, rows, depth), BF16),
            pltpu.VMEM((2 * steps, eighths, depth, columns), BF16),
            pltpu.VMEM((2, rows, out_columns), BF16),
            pltpu.SemaphoreType.DMA((len(chunks) + 1,)),
            pltpu.SemaphoreType.DMA((2,)),
        ],
        cost_estimate=pl.CostEstimate(
            flops=4 * rows * eighths * depth * out_columns,
            transcendentals=0,
            bytes_accessed=22 << 20,
        ),
        compiler_params=pltpu.CompilerParams(vmem_limit_bytes=40 << 20),
        name="project",
    )(info, acc, total, own_weight, *flat)


def grid_width(groups):
    return 1 << ((groups.bit_length() - 1) // 2)


def local(query_states, key_states, value_rows, positions, out_weight):
    tokens, query_heads, head_size = query_states.shape
    kv_heads = key_states.shape[1]
    half = tokens // 2
    ring = lax.axis_size("ctx")
    steps = ring // 2
    groups = lax.axis_size("groups")
    across = grid_width(groups)
    depth = out_weight.shape[0] // 8

    def along(value, by):
        return lax.ppermute(value, "ctx", [(i, (i + by) % ring) for i in range(ring)])

    def beside(value, flip):
        return lax.ppermute(value, "groups", [(i, i ^ flip) for i in range(groups)])

    place = lax.axis_index("groups")
    spot = (place // across) % 2 * 2 + place % 2
    info = jnp.stack(
        [lax.axis_index("ctx"), lax.axis_index("tp"), spot]
    ).astype(jnp.int32)
    own = positions[:1] // half
    tag = jnp.broadcast_to(own.astype(BF16)[:, None], (TAG_ROWS, head_size))
    eighths = out_weight.reshape(8, depth, out_weight.shape[1])
    quarter = lax.dynamic_slice_in_dim(eighths, spot * 2, 2, 0)
    parts = [(key_states[:, h], value_rows[:, h], tag) for h in range(kv_heads)]
    pack = jnp.concatenate([*sum(parts, ()), quarter[0], quarter[1]], axis=0)
    weight_at = pack.shape[0] - 2 * depth
    per = query_heads // kv_heads
    grouped = query_states.reshape(2, half, kv_heads, per, head_size)
    grouped = jnp.transpose(grouped, (2, 0, 3, 1, 4)).reshape(kv_heads, -1, head_size)

    def attending(state, blocks):
        return attend(own, grouped, state, blocks, half)

    ahead = behind = pack
    state = None
    chunks, pieces, sent = [], [], None
    waiting = []
    unattended = []
    begun = 1

    def relay(sent):
        own_part, x_part, y_part, _ = sent
        x_relay = beside(y_part[0], 1)
        y_relay = beside(x_part[1], across)
        pieces.append((own_part, x_part, y_part, x_relay, y_relay))

    for s in range(1, steps + 2):
        if s <= steps:
            ahead = along(ahead, 1)
            if s < steps:
                behind = along(behind, -1)
        done = s - 1
        if done in chunk_ends(steps):
            k = len(chunks)
            came = [*waiting[0], *waiting[1]]
            own_part = jnp.stack(
                [
                    jnp.stack([p[weight_at + h * depth :][:depth] for p in came])
                    for h in range(2)
                ]
            )
            x_part = beside(own_part, 1)
            y_part = beside(own_part, across)
            if sent is not None:
                relay(sent)
            sent = (own_part, x_part, y_part, k)
            chunks.append((begun, done))
            begun = done + 1
            waiting = []
        if done == 0:
            state = attending(None, [pack])
        elif done in batch_ends(steps):
            state = attending(state, unattended)
            unattended = []
        if s <= steps:
            if not waiting:
                waiting = ([], [])
            waiting[0].append(ahead)
            unattended.append(ahead)
            if s < steps:
                waiting[1].append(behind)
                unattended.append(behind)
    relay(sent)
    mine, theirs = project(info, state, eighths, pieces, chunks, steps, ring)
    cores = lax.axis_size("tp")
    arrived = lax.ppermute(theirs, "tp", [(i, (i + 1) % cores) for i in range(cores)])
    return (mine.astype(F32) + arrived.astype(F32)).astype(BF16)


def solution(mesh):
    in_specs = (
        P(("groups", "ctx"), "tp", None),
        P(("groups", "ctx"), "tp", None),
        P(("groups", "ctx"), "tp", None),
        P(("groups", "ctx")),
        P("tp", "ctx"),
    )
    out_specs = P(("groups", "ctx"), "tp")

    return jax.shard_map(local, mesh=mesh, in_specs=in_specs, out_specs=out_specs, check_vma=False)
```

```python
import functools
import math

import jax
import jax.numpy as jnp
from jax import lax
from jax.experimental import pallas as pl
from jax.experimental.pallas import tpu as pltpu
from jax.sharding import PartitionSpec as P


LOW_START = -1e30
TAG_ROWS = 16
LANES = 256
BF16 = jnp.bfloat16
F32 = jnp.float32


def chunk_ends(steps):
    return [*range(1, steps - 2, 3), steps - 1, steps]


def batch_ends(steps):
    return [*range(2, steps - 1, 2), steps - 1, steps]


def pack_kernel(own_ref, spot_ref, keys, values, weight, out, sem):
    tokens, wide = keys.shape
    width = out.shape[1]
    half = tokens // 2
    depth = weight.shape[1]
    rows = 2 * tokens + TAG_ROWS
    heads = wide // width
    copies = [
        pltpu.make_async_copy(
            weight.at[spot_ref[0] * 2 + part],
            out.at[pl.ds(heads * rows + part * depth, depth)],
            sem.at[part],
        )
        for part in range(2)
    ]
    for copy in copies:
        copy.start()
    tag = jnp.full((TAG_ROWS, width), own_ref[0].astype(F32), F32).astype(BF16)
    for h in range(heads):
        at = pl.ds(h * width, width)
        out[pl.ds(h * rows, tokens), :] = keys[:, at]
        for part in range(2):
            value = values[pl.ds(part * half, half), at].astype(F32)
            out[pl.ds(h * rows + tokens + part * half, half), :] = value.T.astype(BF16)
        out[pl.ds(h * rows + 2 * tokens, TAG_ROWS), :] = tag
    for copy in copies:
        copy.wait()


def turn_kernel(queries, out):
    heads, width, lanes = out.shape
    half = queries.shape[0] // 2
    per = lanes // (2 * half)
    for h in range(heads):
        for part in range(2):
            for g in range(per):
                head = h * per + g
                value = queries[pl.ds(part * half, half), pl.ds(head * width, width)]
                out[h, :, pl.ds((part * per + g) * half, half)] = (
                    value.astype(F32).T.astype(BF16)
                )


def gather_kernel(count, at, depth, *refs):
    packs, out, sem = refs[:count], refs[count], refs[count + 1]
    copies = [
        pltpu.make_async_copy(
            packs[n].at[pl.ds(at + part * depth, depth)], out.at[part, n], sem.at[part, n]
        )
        for part in range(2)
        for n in range(count)
    ]
    for copy in copies:
        copy.start()
    for copy in copies:
        copy.wait()


def gather(packs, at, depth):
    count, width = len(packs), packs[0].shape[1]
    anywhere = pl.BlockSpec(memory_space=pl.ANY)
    return pl.pallas_call(
        functools.partial(gather_kernel, count, at, depth),
        in_specs=[anywhere] * count,
        out_specs=anywhere,
        out_shape=jax.ShapeDtypeStruct((2, count, depth, width), BF16),
        scratch_shapes=[pltpu.SemaphoreType.DMA((2, count))],
        compiler_params=pltpu.CompilerParams(vmem_limit_bytes=4 << 20),
        name="gather",
    )(*packs)


def attend_kernel(first, blocks, half, scale, *refs):
    own_ref, q_ref = refs[:2]
    at = 2
    if not first:
        acc_in, max_in, sum_in = refs[at : at + 3]
        at += 3
    packs = refs[at : at + blocks]
    at += blocks
    acc, largest, total, held, sem = refs[at:]
    head = pl.program_id(0)
    rows = held.shape[2]
    span = q_ref.shape[2] // 2

    def copy(h, b):
        return pltpu.make_async_copy(
            packs[b].at[pl.ds(h * rows, rows)], held.at[h, b], sem.at[h, b]
        )

    @pl.when(head == 0)
    def _():
        for h in range(2):
            for b in range(blocks):
                copy(h, b).start()

    if first:
        acc[...] = jnp.zeros_like(acc)
        largest[...] = jnp.full_like(largest, LOW_START)
        total[...] = jnp.zeros_like(total)
    else:
        acc[...] = acc_in[...]
        largest[...] = max_in[...]
        total[...] = sum_in[...]

    for h in range(2):

        @pl.when(head == h)
        def _():
            for b in range(blocks):
                copy(h, b).wait()

    def update(tiles, mask=None):
        found = []
        for start, keys, values in tiles:
            lanes = pl.ds(pl.multiple_of(start, LANES), LANES)
            scores = lax.dot_general(
                keys, q_ref[0, :, lanes], (((1,), (0,)), ((), ())), preferred_element_type=F32
            )
            if mask is not None:
                scores = jnp.where(mask, scores, LOW_START)
            old = largest[0, 0:1, lanes]
            new = jnp.maximum(old, jnp.max(scores, axis=0, keepdims=True))
            factor = jnp.exp2((old - new) * scale)
            weights = jnp.exp2((scores - new) * scale)
            summed = total[0, :, lanes] * factor + jnp.sum(
                weights.reshape(weights.shape[0] // 8, 8, LANES), axis=0
            )
            weighted = acc[0, :, lanes] * factor + lax.dot_general(
                values,
                weights.astype(BF16),
                (((1,), (0,)), ((), ())),
                preferred_element_type=F32,
            )
            found.append((lanes, summed, weighted, jnp.broadcast_to(new, (8, LANES))))
        for lanes, summed, weighted, new in found:
            total[0, :, lanes] = summed
            acc[0, :, lanes] = weighted
            largest[0, :, lanes] = new

    low, high = pl.ds(0, half), pl.ds(half, half)
    vlow, vhigh = pl.ds(2 * half, half), pl.ds(3 * half, half)
    tiles = span // LANES
    if first:
        mine = held.at[head, 0]
        place_k = lax.broadcasted_iota(jnp.int32, (half, LANES), 0)
        place_q = lax.broadcasted_iota(jnp.int32, (half, LANES), 1) % half
        mask = place_k <= place_q

        def visit_own(j, carry):
            at = j * LANES
            update([(at, mine[low], mine[vlow]), (span + at, mine[high], mine[vhigh])], mask)
            update([(span + at, mine[low], mine[vlow])])
            return carry

        lax.fori_loop(0, tiles, visit_own, 0)
        return

    def visit(b, carry):
        block = held.at[head, b]
        tag = jnp.max(block[pl.ds(4 * half, TAG_ROWS)].astype(F32))
        ahead = tag < own_ref[0].astype(F32)
        key_at = pl.multiple_of(jnp.where(ahead, 0, half), half)
        lane_at = jnp.where(ahead, 0, span)

        def some(i, carry):
            work = []
            for j in range(tiles // 2):
                near = (i * (tiles // 2) + j) * LANES
                far = ((1 - i) * (tiles // 2) + j) * LANES
                work.append((span + near, block[low], block[vlow]))
                work.append(
                    (
                        lane_at + far,
                        block[pl.ds(key_at, half)],
                        block[pl.ds(2 * half + key_at, half)],
                    )
                )
            update(work)
            return carry

        return lax.fori_loop(0, 2, some, carry)

    lax.fori_loop(0, blocks, visit, 0)


def attend(own, grouped, state, packs, half):
    first = state is None
    heads, width, lanes = grouped.shape
    blocks = len(packs)
    per_head = lambda *dims: pl.BlockSpec((1, *dims), lambda h: (h, 0, 0))
    anywhere = pl.BlockSpec(memory_space=pl.ANY)
    state_specs = [per_head(width, lanes), per_head(8, lanes), per_head(8, lanes)]
    state_shapes = [
        jax.ShapeDtypeStruct((heads, width, lanes), F32),
        jax.ShapeDtypeStruct((heads, 8, lanes), F32),
        jax.ShapeDtypeStruct((heads, 8, lanes), F32),
    ]
    rows = 4 * half + TAG_ROWS
    flops = heads * blocks * 2 * half * (lanes // 2) * width * 4
    return pl.pallas_call(
        functools.partial(attend_kernel, first, blocks, half, width**-0.5 * math.log2(math.e)),
        grid=(heads,),
        in_specs=[pl.BlockSpec(memory_space=pltpu.SMEM), per_head(width, lanes)]
        + ([] if first else state_specs)
        + [anywhere] * blocks,
        out_specs=state_specs,
        out_shape=state_shapes,
        scratch_shapes=[
            pltpu.VMEM((heads, blocks, rows, width), BF16),
            pltpu.SemaphoreType.DMA((heads, blocks)),
        ],
        input_output_aliases={} if first else {2: 0, 3: 1, 4: 2},
        cost_estimate=pl.CostEstimate(
            flops=flops, transcendentals=flops // (4 * width), bytes_accessed=6 << 20
        ),
        compiler_params=pltpu.CompilerParams(
            vmem_limit_bytes=24 << 20, dimension_semantics=("arbitrary",)
        ),
    )(own, grouped, *(() if first else state), *packs)


def project_kernel(chunks, steps, ring, *refs):
    info, acc, total, own_weight = refs[:4]
    pieces = refs[4 : 4 + 5 * len(chunks)]
    mine, theirs, attended, weights, out, sem, out_sem = refs[4 + 5 * len(chunks) :]
    me, core, spot = info[0], info[1], info[2]
    eighths, rows, depth = attended.shape
    width = weights.shape[-1]
    half = rows // 2
    quarter = [spot, spot ^ 1, spot ^ 2, spot ^ 3]

    def copies(k):
        first_step, last_step = chunks[k]
        forward = last_step - first_step + 1
        backward = min(last_step, steps - 1) - first_step + 1
        own_part, x_part, y_part, x_relay, y_relay = pieces[5 * k : 5 * k + 5]
        found = []
        for source, q, parts in [
            (own_part, 0, (0, 1)),
            (x_part, 1, (0, 1)),
            (y_part, 2, (0, 1)),
            (x_relay, 3, (0,)),
            (y_relay, 3, (1,)),
        ]:
            for part in parts:
                for n, at, to in (
                    (forward, 0, first_step - 1),
                    (backward, forward, steps + first_step - 1),
                ):
                    if n:
                        held = source.at[part] if len(parts) == 2 else source
                        found.append(
                            pltpu.make_async_copy(
                                held.at[pl.ds(at, n)],
                                weights.at[pl.ds(to, n), quarter[q] * 2 + part],
                                sem.at[k],
                            )
                        )
        return found

    own_copy = pltpu.make_async_copy(own_weight, weights.at[2 * steps - 1], sem.at[len(chunks)])
    own_copy.start()
    for k in range(len(chunks)):
        for copy in copies(k):
            copy.start()

    heads, _, lanes = acc.shape
    span = lanes // 2
    for h in range(heads):
        for s in range(2):
            for g in range(span // half):
                at = pl.ds(s * span + g * half, half)
                whole = jnp.sum(total[h, :, at], axis=0, keepdims=True)
                value = (acc[h, :, at] / whole).T.astype(BF16)
                head = h * (span // half) + g
                per = depth // value.shape[1]
                attended[
                    head // per,
                    pl.ds(s * half, half),
                    pl.ds((head % per) * value.shape[1], value.shape[1]),
                ] = value
    own_copy.wait()

    def step(i, carry):
        for k, (first_step, _) in enumerate(chunks):

            @pl.when(i == first_step - 1)
            def _():
                for copy in copies(k):
                    copy.wait()

        summed = jnp.zeros((rows, 2 * width), F32)
        for e in range(eighths):
            both = jnp.concatenate([weights[i, e], weights[steps + i, e]], axis=1)
            summed += jnp.dot(attended[e], both, preferred_element_type=F32)
        rounded = summed.astype(BF16)
        ahead = lax.rem(me - (i + 1) + ring, ring)
        behind = jnp.where(i == steps - 1, me, lax.rem(me + i + 1, ring))
        for value, block in ((rounded[:, :width], ahead), (rounded[:, width:], behind)):
            side = block // (ring // 2)
            at = pl.multiple_of((block - side * (ring // 2)) * width, width)
            out[side ^ core, :, pl.ds(at, width)] = value
        return carry

    lax.fori_loop(0, steps, step, 0)
    done = [
        pltpu.make_async_copy(out.at[0], mine, out_sem.at[0]),
        pltpu.make_async_copy(out.at[1], theirs, out_sem.at[1]),
    ]
    for copy in done:
        copy.start()
    for copy in done:
        copy.wait()


def project(info, state, own_weight, pieces, chunks, steps, ring):
    acc, _, total = state
    heads, width, lanes = acc.shape
    eighths, depth, columns = own_weight.shape
    rows = heads * lanes * width // (eighths * depth)
    out_columns = columns * ring // 2
    anywhere = pl.BlockSpec(memory_space=pl.ANY)
    vmem = pl.BlockSpec(memory_space=pltpu.VMEM)
    flat = [array for chunk in pieces for array in chunk]
    return pl.pallas_call(
        functools.partial(project_kernel, chunks, steps, ring),
        in_specs=[pl.BlockSpec(memory_space=pltpu.SMEM), vmem, vmem]
        + [anywhere] * (1 + len(flat)),
        out_specs=[anywhere, anywhere],
        out_shape=[jax.ShapeDtypeStruct((rows, out_columns), BF16)] * 2,
        scratch_shapes=[
            pltpu.VMEM((eighths, rows, depth), BF16),
            pltpu.VMEM((2 * steps, eighths, depth, columns), BF16),
            pltpu.VMEM((2, rows, out_columns), BF16),
            pltpu.SemaphoreType.DMA((len(chunks) + 1,)),
            pltpu.SemaphoreType.DMA((2,)),
        ],
        cost_estimate=pl.CostEstimate(
            flops=4 * rows * eighths * depth * out_columns,
            transcendentals=0,
            bytes_accessed=22 << 20,
        ),
        compiler_params=pltpu.CompilerParams(vmem_limit_bytes=40 << 20),
        name="project",
    )(info, acc, total, own_weight, *flat)


def grid_width(groups):
    return 1 << ((groups.bit_length() - 1) // 2)


def local(query_states, key_states, value_rows, positions, out_weight):
    tokens, query_heads, head_size = query_states.shape
    kv_heads = key_states.shape[1]
    half = tokens // 2
    ring = lax.axis_size("ctx")
    steps = ring // 2
    groups = lax.axis_size("groups")
    across = grid_width(groups)
    depth = out_weight.shape[0] // 8

    def along(value, by):
        return lax.ppermute(value, "ctx", [(i, (i + by) % ring) for i in range(ring)])

    def beside(value, flip):
        return lax.ppermute(value, "groups", [(i, i ^ flip) for i in range(groups)])

    place = lax.axis_index("groups")
    spot = (place // across) % 2 * 2 + place % 2
    info = jnp.stack(
        [lax.axis_index("ctx"), lax.axis_index("tp"), spot]
    ).astype(jnp.int32)
    own = positions[:1] // half
    eighths = out_weight.reshape(8, depth, out_weight.shape[1])
    smem = pl.BlockSpec(memory_space=pltpu.SMEM)
    vmem = pl.BlockSpec(memory_space=pltpu.VMEM)
    anywhere = pl.BlockSpec(memory_space=pl.ANY)
    weight_at = kv_heads * (2 * tokens + TAG_ROWS)
    pack = pl.pallas_call(
        pack_kernel,
        in_specs=[smem, smem, vmem, vmem, anywhere],
        out_specs=vmem,
        out_shape=jax.ShapeDtypeStruct((weight_at + 2 * depth, head_size), BF16),
        scratch_shapes=[pltpu.SemaphoreType.DMA((2,))],
        compiler_params=pltpu.CompilerParams(vmem_limit_bytes=8 << 20),
        name="pack",
    )(
        own,
        spot[None].astype(jnp.int32),
        key_states.reshape(tokens, -1),
        value_rows.reshape(tokens, -1),
        eighths,
    )
    per = query_heads // kv_heads
    grouped = pl.pallas_call(
        turn_kernel,
        in_specs=[vmem],
        out_specs=vmem,
        out_shape=jax.ShapeDtypeStruct((kv_heads, head_size, per * tokens), BF16),
        compiler_params=pltpu.CompilerParams(vmem_limit_bytes=8 << 20),
        name="turn",
    )(query_states.reshape(tokens, -1))

    def attending(state, blocks):
        return attend(own, grouped, state, blocks, half)

    ahead = behind = pack
    state = None
    chunks, pieces, sent = [], [], None
    waiting = []
    unattended = []
    begun = 1

    def relay(sent):
        own_part, x_part, y_part, _ = sent
        x_relay = beside(y_part[0], 1)
        y_relay = beside(x_part[1], across)
        pieces.append((own_part, x_part, y_part, x_relay, y_relay))

    for s in range(1, steps + 2):
        if s <= steps:
            ahead = along(ahead, 1)
            if s < steps:
                behind = along(behind, -1)
        done = s - 1
        if done in chunk_ends(steps):
            k = len(chunks)
            came = [*waiting[0], *waiting[1]]
            own_part = gather(came, weight_at, depth)
            x_part = beside(own_part, 1)
            y_part = beside(own_part, across)
            if sent is not None:
                relay(sent)
            sent = (own_part, x_part, y_part, k)
            chunks.append((begun, done))
            begun = done + 1
            waiting = []
        if done == 0:
            state = attending(None, [pack])
        elif done in batch_ends(steps):
            state = attending(state, unattended)
            unattended = []
        if s <= steps:
            if not waiting:
                waiting = ([], [])
            waiting[0].append(ahead)
            unattended.append(ahead)
            if s < steps:
                waiting[1].append(behind)
                unattended.append(behind)
    relay(sent)
    mine, theirs = project(info, state, eighths, pieces, chunks, steps, ring)
    cores = lax.axis_size("tp")
    arrived = lax.ppermute(theirs, "tp", [(i, (i + 1) % cores) for i in range(cores)])
    return (mine.astype(F32) + arrived.astype(F32)).astype(BF16)


def solution(mesh):
    in_specs = (
        P(("groups", "ctx"), "tp", None),
        P(("groups", "ctx"), "tp", None),
        P(("groups", "ctx"), "tp", None),
        P(("groups", "ctx")),
        P("tp", "ctx"),
    )
    out_specs = P(("groups", "ctx"), "tp")

    return jax.shard_map(local, mesh=mesh, in_specs=in_specs, out_specs=out_specs, check_vma=False)
```
